32 devices in a mesh: groups: 2 (over y), ep: 4 (over z), tp: 2 (over x), dp: 2 (over core).
Axes of the slice: x: 2, y: 2, z: 4, core: 2. Of those that a mesh axis runs over, the one named last changes fastest.
Arguments:
- tokens: bfloat16 [256, 5120], P(('groups', 'ep', 'tp', 'dp')), parts along dimension 0, may hold values from -6 to 6
- route_weights: float32 [256, 8], P(('groups', 'ep', 'tp', 'dp')), parts along dimension 0, may hold values from 0.1 to 1
- expert_ids: int32 [256, 8], P(('groups', 'ep', 'tp', 'dp')), parts along dimension 0, may hold values from 0 to 31, all different within a row; in each aligned block of 8 rows (0 to 7, 8 to 15, ...) at most 4 rows name the same one
- gate_weight: bfloat16 [32, 5120, 1024], P('ep', None, ('tp', 'dp')), may hold values from -0.078125 to 0.078125
- up_weight: bfloat16 [32, 5120, 1024], P('ep', None, ('tp', 'dp')), may hold values from -0.078125 to 0.078125
- down_weight: bfloat16 [32, 1024, 5120], P('ep', None, ('tp', 'dp')), may hold values from -0.1875 to 0.1875
Outputs:
- combined: bfloat16 [256, 5120], P(('groups', 'ep', 'tp', 'dp')), parts along dimension 0
The draws below stay inside these ranges and needn't reach their ends.
There are 2 independent parts, one for each index of `groups`. The reference program is written for one: setup_inputs(seed, part) draws one part's arguments, and reference() takes and returns one part's arrays. A program takes and returns all parts, laid end to end along the dimension named above; an argument that names none is the same for every part. Nothing has to cross between parts.
Inputs may be any that keep to these rules, and one draw needn't show every extreme that they name: `expert_ids`: each row names 8 different experts. Among the 8 rows of one device no expert is named more than 4 times, and in every draw some device's rows name some expert exactly 4 times.
All inputs are finite; a program needn't handle non-finite values.
Results may differ from the reference program's by a relative error of at most 0.0057.
Values may be sent and summed in bfloat16 or wider, within the bound.
A program may use at most 128 MiB of HBM per device.

```python
import math
import jax
import jax.numpy as jnp
import numpy as np
from jax import lax

D = 5120
FF = 1024
EXPERTS = 32
TOP = 8
TOK_DEV = 8
CAP = 4
TOKENS = 128
N_EP = 4
N_TP = 2
N_DP = 2


def block_levels(own_key, dims, shards, low, top_value):
    gain = 1.0
    for dim, shards_of in shards:
        heights = jax.random.uniform(jax.random.fold_in(jax.random.fold_in(own_key, 6), dim), (shards_of,), jnp.float32, low / len(shards), top_value / len(shards))
        gain = gain * jnp.repeat(jnp.exp(heights), dims[dim] // shards_of).reshape((-1,) + (1,) * (len(dims) - 1 - dim))
    return gain


def deal_out(key, own, number, rows, count, top, most, lean):
    sequence = jax.random.permutation(key, count)
    heavy_load, usual = portions_of(count, rows * top, most, lean, True), portions_of(count, rows * top, most, lean, False)
    places = jnp.arange(count)

    def named(tallies, turn):
        used = int((tallies > 0).sum())
        fixed = max(1, used // 4)
        passed = fixed + (places - fixed + turn * (used - fixed)) % max(1, count - fixed)
        return jnp.zeros((count,), jnp.int32).at[sequence[jnp.where(places < fixed, places, passed)]].set(jnp.asarray(tallies, jnp.int32))

    tallies = jnp.where(number % 4 == 0, named(heavy_load, number // 4), named(usual, number - number // 4 - 1))
    mixed = jax.random.permutation(jax.random.fold_in(own, 3), count)
    donor, sink = mixed[0:count // 2 * 2:2], mixed[1:count // 2 * 2:2]
    slack = jnp.minimum(tallies[donor] - 1, most - tallies[sink]) // 2
    slack = jnp.where((donor == sequence[0]) | (sink == sequence[0]) | (tallies[sink] == 0), 0, jnp.maximum(slack, 0))
    passed = jax.random.randint(jax.random.fold_in(own, 4), (count // 2,), 0, 1 << 20) % (slack + 1)
    tallies = tallies.at[donor].add(-passed).at[sink].add(passed)
    members = jnp.searchsorted(jnp.cumsum(tallies), jnp.arange(rows * top), side="right").astype(jnp.int32)
    grid = members.reshape(top, rows).T
    grid = grid[jax.random.permutation(jax.random.fold_in(own, 1), rows)]
    turn = jax.random.randint(jax.random.fold_in(own, 2), (rows, 1), 0, top)
    return jnp.take_along_axis(grid, (jnp.arange(top)[None, :] + turn) % top, axis=1)


def portions_of(number_of, total, most, lean, full):
    weights = [(1 << 20) // math.isqrt(rank ** lean) + 1 for rank in range(1, number_of + 1)]
    largest = most if full else min(most, max(-(-total // number_of), total * weights[0] // sum(weights)))
    least = 1 if total - largest >= number_of - 1 else 0
    given, spare = [largest] + [least] * (number_of - 1), total - largest - least * (number_of - 1)
    while spare > 0:
        candidates = [i for i in range(1, number_of) if given[i] < largest] or [i for i in range(1, number_of) if given[i] < most]
        mass, budget = sum([weights[i] for i in candidates]), spare
        for i in candidates:
            extra = min(most - given[i], max(1, budget * weights[i] // mass), spare)
            given[i] = given[i] + extra
            spare = spare - extra
    return np.array(given)


def normal_values(stream_key, dims, deviation, limit, shards=(), held_as=jnp.bfloat16):
    array = jax.random.normal(stream_key, dims, jnp.float32) * deviation
    if len(shards) > 0:
        array = block_levels(stream_key, dims, shards, -0.22, 0.18) * array
    return jnp.clip(array, min=-limit, max=limit).astype(held_as)


def setup_inputs(seed: int = 0, part: int = 0) -> dict:
    streams_of = jax.random.split(jax.random.key(seed), 7)
    own_keys = jax.random.split(jax.random.fold_in(streams_of[6], part), 7)
    tokens = normal_values(own_keys[0], (TOKENS, D), 1.0, 6.0, ((0, 16),))
    route_weights = jnp.clip(jnp.exp(math.log(1.0) - 2.3025851 * jax.random.uniform(own_keys[1], (TOKENS, TOP), jnp.float32) ** block_levels(own_keys[1], (TOKENS, TOP), ((0, 16),), -0.2, 0.2)), 0.1, 1.0)
    expert_ids_keys = jax.random.split(jax.random.fold_in(own_keys[2], 1), TOKENS // TOK_DEV)
    expert_ids_turns = jax.random.permutation(jax.random.fold_in(own_keys[2], 3), TOKENS // TOK_DEV)
    expert_ids = jax.vmap(lambda own, number: deal_out(jax.random.fold_in(own_keys[2], 2), own, number, TOK_DEV, EXPERTS, TOP, CAP, 2))(expert_ids_keys, expert_ids_turns).reshape((TOKENS, TOP))
    gate_weight = normal_values(streams_of[3], (EXPERTS, D, FF), D ** -0.5, 0.078125, ((0, 4), (2, 4)))
    up_weight = normal_values(streams_of[4], (EXPERTS, D, FF), D ** -0.5, 0.078125, ((0, 4), (2, 4)))
    down_weight = normal_values(streams_of[5], (EXPERTS, FF, D), FF ** -0.5, 0.1875, ((0, 4), (2, 4)))
    return dict(tokens=tokens, route_weights=route_weights, expert_ids=expert_ids, gate_weight=gate_weight, up_weight=up_weight, down_weight=down_weight)


def reference(tokens, route_weights, expert_ids, gate_weight, up_weight, down_weight):
    devices = N_EP * N_TP * N_DP
    blocks = expert_ids.reshape(devices, TOK_DEV * TOP)
    onehot = (blocks[:, :, None] == jnp.arange(EXPERTS, dtype=jnp.int32)[None, None, :]).astype(jnp.int32)
    slots = jnp.sum(onehot * jnp.cumsum(onehot, axis=1), axis=2) - 1
    device_ids = jnp.arange(devices, dtype=jnp.int32)[:, None]
    position = (device_ids * CAP + slots).reshape(-1).astype(jnp.int32)
    flat_ids = expert_ids.reshape(-1).astype(jnp.int32)
    owner = (jnp.arange(TOKENS * TOP, dtype=jnp.int32) // TOP).astype(jnp.int32)
    span = devices * CAP

    def one_expert(expert):
        index = jnp.where(flat_ids == expert, position, span).astype(jnp.int32)
        table = jnp.full((span,), TOKENS, jnp.int32).at[index].set(owner, mode="drop")
        rows = jnp.take(tokens, table, axis=0, mode="fill", fill_value=0)
        gate = jnp.dot(rows, gate_weight[expert], preferred_element_type=jnp.float32)
        up = jnp.dot(rows, up_weight[expert], preferred_element_type=jnp.float32)
        hidden = (jax.nn.silu(gate) * up).astype(jnp.bfloat16)
        return jnp.dot(hidden, down_weight[expert], preferred_element_type=jnp.float32).astype(jnp.bfloat16)

    outputs = lax.map(one_expert, jnp.arange(EXPERTS, dtype=jnp.int32))
    flat_out = outputs.reshape(EXPERTS * span, D)
    picked_index = (flat_ids * span + position).reshape(TOKENS, TOP).astype(jnp.int32)
    total = jnp.zeros((TOKENS, D), jnp.float32)
    for route in range(TOP):
        chosen = jnp.take(flat_out, picked_index[:, route], axis=0).astype(jnp.float32)
        total = total + route_weights[:, route:route + 1] * chosen
    return total.astype(jnp.bfloat16)
```

```python
import functools

import jax
import jax.numpy as jnp
from jax import lax
from jax.experimental import pallas as pl
from jax.experimental.pallas import tpu as pltpu
from jax.sharding import PartitionSpec as P

MESH = pl.DeviceIdType.MESH
LANES = 128
CHUNKS = 2
SLOTS = 12


def routed_rows(tokens, route_weights, expert_ids, experts, chunks, ext):
    lane = jnp.arange(experts, dtype=jnp.int32)
    dense = jnp.sum(
        jnp.where(expert_ids[:, :, None] == lane, route_weights[:, :, None], 0.0), axis=1
    )
    first = lax.reduce_precision(dense, 8, 7)
    second = lax.reduce_precision(dense - first, 8, 7)
    third = dense - first - second
    side = jnp.concatenate([first, second, third], axis=1).astype(jnp.bfloat16)
    side = jnp.pad(side, ((0, 0), (0, ext - side.shape[1])))
    rows, width = tokens.shape
    depth = width // chunks
    return jnp.stack(
        [
            jnp.concatenate([tokens[:, k * depth : (k + 1) * depth], side], axis=1)
            for k in range(chunks)
        ]
    )


def kernel(
    dims,
    xin,
    gate_hbm,
    up_hbm,
    down_hbm,
    out,
    xr,
    x2,
    gbuf,
    ubuf,
    dbuf,
    acc,
    hid,
    pbuf,
    back,
    g_sem,
    u_sem,
    d_sem,
    own_sem,
    xs_sem,
    xr_sem,
    hs_sem,
    hr_sem,
    ps_sem,
    pr_sem,
):
    n_ep, n_tp, n_dp, experts = dims
    nq = n_tp * n_dp
    nb = n_ep * nq
    chunks, _, rows, _ = xr.shape
    _, count, depth = x2.shape
    slots = gbuf.shape[0]
    local = acc.shape[0]
    ff = gbuf.shape[2]
    tiles, _, full, tile = dbuf.shape
    units = chunks * local
    mt = min(count, 128)
    mb = mt // rows
    msteps = count // mt

    z, x, c = lax.axis_index("ep"), lax.axis_index("tp"), lax.axis_index("dp")
    q = x * n_dp + c
    me = z * nq + q

    def weights_in(u):
        k, e = u // local, u % local
        s = u % slots
        span = pl.ds(pl.multiple_of(k * depth, depth), depth)
        return (
            pltpu.make_async_copy(gate_hbm.at[e, span, :], gbuf.at[s], g_sem.at[s]),
            pltpu.make_async_copy(up_hbm.at[e, span, :], ubuf.at[s], u_sem.at[s]),
        )

    def down_in(j):
        return pltpu.make_async_copy(
            down_hbm.at[:, :, j * tile : (j + 1) * tile], dbuf.at[j], d_sem.at[j]
        )

    for u in range(min(slots, units)):
        for copy in weights_in(u):
            copy.start()
    if units <= slots:
        for j in range(tiles):
            down_in(j).start()
    own = pltpu.make_async_copy(xin, xr.at[:, me], own_sem)
    own.start()

    barrier = pltpu.get_barrier_semaphore()

    def others(act):
        for dz in range(n_ep):
            for dx in range(n_tp):
                for dc in range(n_dp):
                    if dz or dx or dc:
                        act(lax.rem(z + dz, n_ep), lax.rem(x + dx, n_tp), lax.rem(c + dc, n_dp))

    others(
        lambda a, b, d: pl.semaphore_signal(
            barrier, inc=1, device_id={"ep": a, "tp": b, "dp": d}, device_id_type=MESH
        )
    )
    pl.semaphore_wait(barrier, nb - 1)

    def pass_block(k, block, src, a, b, d):
        pltpu.make_async_remote_copy(
            src_ref=src,
            dst_ref=xr.at[k, block],
            send_sem=xs_sem.at[k],
            recv_sem=xr_sem.at[k, block],
            device_id={"ep": a, "tp": b, "dp": d},
            device_id_type=MESH,
        ).start()

    def arrived(k, block):
        pltpu.make_async_copy(xr.at[k, block], xr.at[k, block], xr_sem.at[k, block]).wait()

    order = []
    for s in range(1, n_ep // 2 + 1):
        order.append(s)
        if n_ep - s != s:
            order.append(n_ep - s)

    def to_tp(k, block, src):
        for dx in range(1, n_tp):
            pass_block(k, block, src, z, lax.rem(x + dx, n_tp), c)

    def to_dp(k, block, src):
        for dc in range(1, n_dp):
            pass_block(k, block, src, z, x, lax.rem(c + dc, n_dp))

    for k in range(chunks):
        for s in order:
            pass_block(k, me, xin.at[k], lax.rem(z + s, n_ep), x, c)
        to_tp(k, me, xin.at[k])
        to_dp(k, me, xin.at[k])

    def ep_steps(k):
        for s in order:
            block = lax.rem(z + n_ep - s, n_ep) * nq + q
            arrived(k, block)
            to_tp(k, block, xr.at[k, block])
            to_dp(k, block, xr.at[k, block])

    def tp_steps(k):
        for s in [0] + order:
            for dx in range(1, n_tp):
                block = lax.rem(z + n_ep - s, n_ep) * nq + lax.rem(x + dx, n_tp) * n_dp + c
                arrived(k, block)
                to_dp(k, block, xr.at[k, block])

    def dp_steps(k):
        for s in [0] + order:
            for dx in range(n_tp):
                for dc in range(1, n_dp):
                    block = (
                        lax.rem(z + n_ep - s, n_ep) * nq
                        + lax.rem(x + dx, n_tp) * n_dp
                        + lax.rem(c + dc, n_dp)
                    )
                    arrived(k, block)

    def each_m(body):
        if msteps == 1:
            body(0)
        else:

            @pl.loop(0, msteps)
            def _(m):
                body(m)

    def repack(k):
        def body(m):
            part = xr[k, pl.ds(m * mb, mb), :, :depth].astype(jnp.float32)
            x2[k, pl.ds(pl.multiple_of(m * mt, mt), mt), :] = part.reshape(mt, depth).astype(
                jnp.bfloat16
            )

        each_m(body)

    def hidden_to(e, qs, b, d):
        cols = pl.ds(pl.multiple_of(qs * ff, ff), ff)
        pltpu.make_async_remote_copy(
            src_ref=hid.at[e, :, cols],
            dst_ref=hid.at[e, :, cols],
            send_sem=hs_sem.at[e],
            recv_sem=hr_sem.at[e, qs],
            device_id={"ep": z, "tp": b, "dp": d},
            device_id_type=MESH,
        ).start()

    def hidden_arrived(e, qs):
        cols = pl.ds(pl.multiple_of(qs * ff, ff), ff)
        pltpu.make_async_copy(hid.at[e, :, cols], hid.at[e, :, cols], hr_sem.at[e, qs]).wait()

    def hidden_relay(e):
        for dx in range(1, n_tp):
            qs = lax.rem(x + dx, n_tp) * n_dp + c
            hidden_arrived(e, qs)
            for dc in range(1, n_dp):
                hidden_to(e, qs, x, lax.rem(c + dc, n_dp))

    def unit(k, e):
        u = k * local + e
        s = lax.rem(u, slots)
        for copy in weights_in(u):
            copy.wait()

        def body(m):
            span = pl.ds(pl.multiple_of(m * mt, mt), mt)
            gate = jnp.dot(x2[k, span, :], gbuf[s], preferred_element_type=jnp.float32)
            up = jnp.dot(x2[k, span, :], ubuf[s], preferred_element_type=jnp.float32)
            if k > 0:
                gate = gate + acc[e, span, :ff]
                up = up + acc[e, span, ff:]
            if k < chunks - 1:
                acc[e, span, :ff] = gate
                acc[e, span, ff:] = up
            else:
                side = xr[k, pl.ds(m * mb, mb), :, depth:].astype(jnp.float32)
                side = side.reshape(mt, side.shape[2])
                lane = lax.broadcasted_iota(jnp.int32, side.shape, 1)
                named = z * local + e
                mine = (lane == named) | (lane == named + experts) | (lane == named + 2 * experts)
                weight = jnp.sum(jnp.where(mine, side, 0.0), axis=1, keepdims=True)
                hidden = gate / (1.0 + jnp.exp(-gate)) * up * weight
                cols = pl.ds(pl.multiple_of(q * ff, ff), ff)
                hid[e, span, cols] = hidden.astype(jnp.bfloat16)

        each_m(body)
        if units > slots:

            @pl.when(u + slots < units)
            def _():
                for copy in weights_in(u + slots):
                    copy.start()

            @pl.when(u == units - slots - 1)
            def _():
                for j in range(tiles):
                    down_in(j).start()

        if k == chunks - 1:
            for dx in range(1, n_tp):
                hidden_to(e, q, lax.rem(x + dx, n_tp), c)
            for dc in range(1, n_dp):
                hidden_to(e, q, x, lax.rem(c + dc, n_dp))

    ep_steps(0)
    tp_steps(0)
    own.wait()
    dp_steps(0)
    repack(0)
    for k in range(chunks):
        last = k == chunks - 1

        @pl.loop(0, local)
        def _(e):
            unit(k, e)
            if not last and local >= 4:
                pl.when(e == 0)(lambda: ep_steps(k + 1))
                pl.when(e == 2)(lambda: tp_steps(k + 1))
            if last:

                @pl.when(e >= 2)
                def _():
                    hidden_relay(e - 2)

        if not last:
            if local < 4:
                ep_steps(k + 1)
                tp_steps(k + 1)
            dp_steps(k + 1)
            repack(k + 1)

    for e in range(max(local - 2, 0), local):
        hidden_relay(e)

    @pl.loop(0, local)
    def _(e):
        for dx in range(n_tp):
            for dc in range(1, n_dp):
                hidden_arrived(e, lax.rem(x + dx, n_tp) * n_dp + lax.rem(c + dc, n_dp))

    for j in range(tiles):
        down_in(j).wait()

        def body(m):
            span = pl.ds(pl.multiple_of(m * mt, mt), mt)

            def add(e, total):
                return total + jnp.dot(
                    hid[e, span, :], dbuf[j, e], preferred_element_type=jnp.float32
                )

            total = lax.fori_loop(0, local, add, jnp.zeros((mt, tile), jnp.float32))
            pbuf[j, pl.ds(m * mb, mb)] = total.reshape(mb, rows, tile).astype(jnp.bfloat16)

        each_m(body)
        pltpu.make_async_copy(pbuf.at[j, me], back.at[j, z, q], pr_sem.at[j]).start()

        def give(a, b, d):
            pltpu.make_async_remote_copy(
                src_ref=pbuf.at[j, a * nq + b * n_dp + d],
                dst_ref=back.at[j, z, q],
                send_sem=ps_sem.at[j],
                recv_sem=pr_sem.at[j],
                device_id={"ep": a, "tp": b, "dp": d},
                device_id_type=MESH,
            ).start()

        others(give)

    for j in range(tiles):
        pltpu.make_async_copy(back.at[j], back.at[j], pr_sem.at[j]).wait()
        for qs in range(nq):
            total = back[j, 0, qs].astype(jnp.float32)
            for a in range(1, n_ep):
                total = total + back[j, a, qs].astype(jnp.float32)
            at = (qs * tiles + j) * tile
            out[:, at : at + tile] = total.astype(jnp.bfloat16)

    for k in range(chunks):
        sent = xr.at[k, pl.ds(0, nb - 1)]
        pltpu.make_async_copy(sent, sent, xs_sem.at[k]).wait()
    for e in range(local):
        sent = hid.at[e, :, pl.ds(0, (nq - 1) * ff)]
        pltpu.make_async_copy(sent, sent, hs_sem.at[e]).wait()
    for j in range(tiles):
        sent = pbuf.at[j, pl.ds(0, nb - 1)]
        pltpu.make_async_copy(sent, sent, ps_sem.at[j]).wait()


def per_device(tokens, route_weights, expert_ids, gate_weight, up_weight, down_weight):
    n_ep, n_tp, n_dp = (lax.axis_size(name) for name in ("ep", "tp", "dp"))
    nq = n_tp * n_dp
    nb = n_ep * nq
    rows, width = tokens.shape
    local, _, ff = gate_weight.shape
    _, full, part = down_weight.shape
    experts = local * n_ep
    ext = -(-3 * experts // LANES) * LANES
    chunks = CHUNKS if width % (CHUNKS * LANES) == 0 else 1
    depth = width // chunks
    slots = min(SLOTS, chunks * local)
    tile = 2 * LANES if part % (2 * LANES) == 0 else LANES
    tiles = part // tile
    count = nb * rows
    xin = routed_rows(tokens, route_weights, expert_ids, experts, chunks, ext)
    any_space = pl.BlockSpec(memory_space=pl.ANY)
    dma = pltpu.SemaphoreType.DMA
    bf16 = jnp.bfloat16
    return pl.pallas_call(
        functools.partial(kernel, (n_ep, n_tp, n_dp, experts)),
        out_shape=jax.ShapeDtypeStruct((rows, width), bf16),
        in_specs=[pl.BlockSpec(memory_space=pltpu.VMEM), any_space, any_space, any_space],
        out_specs=pl.BlockSpec(memory_space=pltpu.VMEM),
        scratch_shapes=[
            pltpu.VMEM((chunks, nb, rows, depth + ext), bf16),
            pltpu.VMEM((chunks, count, depth), bf16),
            pltpu.VMEM((slots, depth, ff), bf16),
            pltpu.VMEM((slots, depth, ff), bf16),
            pltpu.VMEM((tiles, local, full, tile), bf16),
            pltpu.VMEM((local, count, 2 * ff), jnp.float32),
            pltpu.VMEM((local, count, full), bf16),
            pltpu.VMEM((tiles, nb, rows, tile), bf16),
            pltpu.VMEM((tiles, n_ep, nq, rows, tile), bf16),
            dma((slots,)),
            dma((slots,)),
            dma((tiles,)),
            dma,
            dma((chunks,)),
            dma((chunks, nb)),
            dma((local,)),
            dma((local, nq)),
            dma((tiles,)),
            dma((tiles,)),
        ],
        compiler_params=pltpu.CompilerParams(
            collective_id=0, has_side_effects=True, vmem_limit_bytes=67043328
        ),
        name="experts",
    )(xin, gate_weight, up_weight, down_weight)


def solution(mesh):
    rows = P(("groups", "ep", "tp", "dp"), None)
    weights = P("ep", None, ("tp", "dp"))
    return jax.shard_map(
        per_device,
        mesh=mesh,
        in_specs=(rows, rows, rows, weights, weights, weights),
        out_specs=rows,
        check_vma=False,
    )
```

```python
import functools

import jax
import jax.numpy as jnp
from jax import lax
from jax.experimental import pallas as pl
from jax.experimental.pallas import tpu as pltpu
from jax.sharding import PartitionSpec as P

MESH = pl.DeviceIdType.MESH
LANES = 128
CHUNKS = 4
SLOTS = 24
CAP = 4


def rows_and_routes(tokens, route_weights, expert_ids, xin, experts):
    chunks, rows, wide = xin.shape
    depth = tokens.shape[1] // chunks
    weight, ids = route_weights[...], expert_ids[...]
    lane = lax.broadcasted_iota(jnp.int32, (rows, wide - depth), 1)
    side = jnp.zeros((rows, wide - depth), jnp.float32)
    for term in range(3):
        held = weight.astype(jnp.bfloat16).astype(jnp.float32)
        weight = weight - held
        for k in range(ids.shape[1]):
            hit = lane == ids[:, k : k + 1] + term * experts
            side = side + jnp.where(hit, held[:, k : k + 1], 0.0)
    for k in range(chunks):
        xin[k, :, :depth] = tokens[:, k * depth : (k + 1) * depth]
        xin[k, :, depth:] = side.astype(jnp.bfloat16)


def kernel(
    dims,
    tokens,
    route_weights,
    expert_ids,
    gate_hbm,
    up_hbm,
    down_hbm,
    out,
    xin,
    xr,
    x2,
    gbuf,
    ubuf,
    dbuf,
    acc,
    packed,
    hid,
    ranks,
    pbuf,
    back,
    g_sem,
    u_sem,
    d_sem,
    own_sem,
    xs_sem,
    xr_sem,
    hs_sem,
    hr_sem,
    ps_sem,
    pr_sem,
):
    n_ep, n_tp, n_dp, experts = dims
    nq = n_tp * n_dp
    nb = n_ep * nq
    chunks, _, rows, _ = xr.shape
    _, count, depth = x2.shape
    slots = gbuf.shape[0]
    local = acc.shape[0]
    ff = gbuf.shape[2]
    tiles, _, full, tile = dbuf.shape
    units = chunks * local
    groups = 2 if local % 4 == 0 else 1
    ge = local // groups
    packed_rows = packed.shape[1]
    mt = min(count, 128)
    mb = mt // rows
    msteps = count // mt
    ms = packed_rows // msteps

    z, x, c = lax.axis_index("ep"), lax.axis_index("tp"), lax.axis_index("dp")
    q = x * n_dp + c
    me = z * nq + q

    def weights_in(u):
        k, e = u % (chunks * ge) // ge, u // (chunks * ge) * ge + u % ge
        s = u % slots
        span = pl.ds(pl.multiple_of(k * depth, depth), depth)
        return (
            pltpu.make_async_copy(gate_hbm.at[e, span, :], gbuf.at[s], g_sem.at[s]),
            pltpu.make_async_copy(up_hbm.at[e, span, :], ubuf.at[s], u_sem.at[s]),
        )

    def down_in(j):
        return pltpu.make_async_copy(
            down_hbm.at[:, :, j * tile : (j + 1) * tile], dbuf.at[j], d_sem.at[j]
        )

    for u in range(min(slots, units)):
        for copy in weights_in(u):
            copy.start()
    if units <= slots:
        for j in range(tiles):
            down_in(j).start()
    rows_and_routes(tokens, route_weights, expert_ids, xin, experts)
    own = pltpu.make_async_copy(xin, xr.at[:, me], own_sem)
    own.start()

    barrier = pltpu.get_barrier_semaphore()

    def others(act):
        for dz in range(n_ep):
            for dx in range(n_tp):
                for dc in range(n_dp):
                    if dz or dx or dc:
                        act(lax.rem(z + dz, n_ep), lax.rem(x + dx, n_tp), lax.rem(c + dc, n_dp))

    others(
        lambda a, b, d: pl.semaphore_signal(
            barrier, inc=1, device_id={"ep": a, "tp": b, "dp": d}, device_id_type=MESH
        )
    )
    pl.semaphore_wait(barrier, nb - 1)

    def pass_block(k, block, src, a, b, d):
        pltpu.make_async_remote_copy(
            src_ref=src,
            dst_ref=xr.at[k, block],
            send_sem=xs_sem.at[k],
            recv_sem=xr_sem.at[k, block],
            device_id={"ep": a, "tp": b, "dp": d},
            device_id_type=MESH,
        ).start()

    def arrived(k, block):
        pltpu.make_async_copy(xr.at[k, block], xr.at[k, block], xr_sem.at[k, block]).wait()

    order = []
    for s in range(1, n_ep // 2 + 1):
        order.append(s)
        if n_ep - s != s:
            order.append(n_ep - s)

    def to_tp(k, block, src):
        for dx in range(1, n_tp):
            pass_block(k, block, src, z, lax.rem(x + dx, n_tp), c)

    def to_dp(k, block, src):
        for dc in range(1, n_dp):
            pass_block(k, block, src, z, x, lax.rem(c + dc, n_dp))

    for k in range(chunks):
        for s in order:
            pass_block(k, me, xin.at[k], lax.rem(z + s, n_ep), x, c)
        to_tp(k, me, xin.at[k])
        to_dp(k, me, xin.at[k])

    def ep_steps(k):
        for s in order:
            block = lax.rem(z + n_ep - s, n_ep) * nq + q
            arrived(k, block)
            to_tp(k, block, xr.at[k, block])
            to_dp(k, block, xr.at[k, block])

    def tp_steps(k):
        for s in [0] + order:
            for dx in range(1, n_tp):
                block = lax.rem(z + n_ep - s, n_ep) * nq + lax.rem(x + dx, n_tp) * n_dp + c
                arrived(k, block)
                to_dp(k, block, xr.at[k, block])

    def dp_steps(k):
        for s in [0] + order:
            for dx in range(n_tp):
                for dc in range(1, n_dp):
                    block = (
                        lax.rem(z + n_ep - s, n_ep) * nq
                        + lax.rem(x + dx, n_tp) * n_dp
                        + lax.rem(c + dc, n_dp)
                    )
                    arrived(k, block)

    def each_m(body):
        if msteps == 1:
            body(0)
        else:

            @pl.loop(0, msteps)
            def _(m):
                body(m)

    def repack(k):
        def body(m):
            part = xr[k, pl.ds(m * mb, mb), :, :depth].astype(jnp.float32)
            x2[k, pl.ds(pl.multiple_of(m * mt, mt), mt), :] = part.reshape(mt, depth).astype(
                jnp.bfloat16
            )

        each_m(body)

    def routes(k, m):
        side = xr[k, pl.ds(m * mb, mb), :, depth:].astype(jnp.float32)
        return side.reshape(mt, side.shape[2])

    def rank_rows(k):
        def body(m):
            named = (routes(k, m) > 0.0).astype(jnp.float32)
            row = lax.broadcasted_iota(jnp.int32, (mt, mt), 0)
            col = lax.broadcasted_iota(jnp.int32, (mt, mt), 1)
            before = (row // rows == col // rows) & (col < row)
            count_before = jnp.dot(
                before.astype(jnp.float32).astype(jnp.bfloat16),
                named.astype(jnp.bfloat16),
                preferred_element_type=jnp.float32,
            )
            ranks[pl.ds(pl.multiple_of(m * mt, mt), mt), :] = jnp.where(
                named > 0.0, count_before, -1.0
            )

        each_m(body)

    def places(e, span):
        table = ranks[span, :]
        lane = lax.broadcasted_iota(jnp.int32, table.shape, 1)
        rank = jnp.sum(jnp.where(lane == z * local + e, table, 0.0), axis=1, keepdims=True)
        row = lax.broadcasted_iota(jnp.int32, (mt, ms), 0)
        slot = lax.broadcasted_iota(jnp.int32, (mt, ms), 1)
        mine = (row // rows == slot // CAP) & ((slot % CAP).astype(jnp.float32) == rank)
        return mine.astype(jnp.float32).astype(jnp.bfloat16)

    def hidden_to(e, qs, b, d):
        cols = pl.ds(pl.multiple_of(qs * ff, ff), ff)
        pltpu.make_async_remote_copy(
            src_ref=packed.at[e, :, cols],
            dst_ref=packed.at[e, :, cols],
            send_sem=hs_sem.at[e],
            recv_sem=hr_sem.at[e, qs],
            device_id={"ep": z, "tp": b, "dp": d},
            device_id_type=MESH,
        ).start()

    def hidden_arrived(e, qs):
        cols = pl.ds(pl.multiple_of(qs * ff, ff), ff)
        pltpu.make_async_copy(packed.at[e, :, cols], packed.at[e, :, cols], hr_sem.at[e, qs]).wait()

    def hidden_relay(e):
        for dx in range(1, n_tp):
            qs = lax.rem(x + dx, n_tp) * n_dp + c
            hidden_arrived(e, qs)
            for dc in range(1, n_dp):
                hidden_to(e, qs, x, lax.rem(c + dc, n_dp))

    def unit(k, e):
        u = e // ge * (chunks * ge) + k * ge + e % ge
        s = lax.rem(u, slots)
        for copy in weights_in(u):
            copy.wait()

        def body(m):
            span = pl.ds(pl.multiple_of(m * mt, mt), mt)
            gate = jnp.dot(x2[k, span, :], gbuf[s], preferred_element_type=jnp.float32)
            up = jnp.dot(x2[k, span, :], ubuf[s], preferred_element_type=jnp.float32)
            if k > 0:
                gate = gate + acc[e, span, :ff]
                up = up + acc[e, span, ff:]
            if k < chunks - 1:
                acc[e, span, :ff] = gate
                acc[e, span, ff:] = up
            else:
                side = routes(k, m)
                named = z * local + e
                lane = lax.broadcasted_iota(jnp.int32, side.shape, 1)
                mine = (lane == named) | (lane == named + experts) | (lane == named + 2 * experts)
                weight = jnp.sum(jnp.where(mine, side, 0.0), axis=1, keepdims=True)
                hidden = gate / (1.0 + jnp.exp(-gate)) * up * weight
                kept = lax.dot_general(
                    places(e, span),
                    hidden.astype(jnp.bfloat16),
                    (((0,), (0,)), ((), ())),
                    preferred_element_type=jnp.float32,
                )
                cols = pl.ds(pl.multiple_of(q * ff, ff), ff)
                slot = pl.ds(pl.multiple_of(m * ms, ms), ms)
                packed[e, slot, cols] = kept.astype(jnp.bfloat16)

        each_m(body)
        if units > slots:

            @pl.when(u + slots < units)
            def _():
                for copy in weights_in(u + slots):
                    copy.start()

            @pl.when(u == units - slots - 1)
            def _():
                for j in range(tiles):
                    down_in(j).start()

        if k == chunks - 1:
            for dx in range(1, n_tp):
                hidden_to(e, q, lax.rem(x + dx, n_tp), c)
            for dc in range(1, n_dp):
                hidden_to(e, q, x, lax.rem(c + dc, n_dp))

    ep_steps(0)
    tp_steps(0)
    own.wait()
    dp_steps(0)
    repack(0)
    rank_rows(0)
    for g in range(groups):
        for k in range(chunks):
            last = k == chunks - 1
            ahead = g == 0 and not last

            @pl.loop(0, ge)
            def _(i):
                unit(k, g * ge + i)
                if ahead and ge >= 4:
                    pl.when(i == 0)(lambda: ep_steps(k + 1))
                    pl.when(i == 2)(lambda: tp_steps(k + 1))
                if g > 0 and k == 0:
                    pl.when(i < 2)(lambda: hidden_relay(g * ge - 2 + i))
                if last and ge >= 2:
                    pl.when(i >= 2)(lambda: hidden_relay(g * ge + i - 2))

            if ahead:
                if ge < 4:
                    ep_steps(k + 1)
                    tp_steps(k + 1)
                dp_steps(k + 1)
                repack(k + 1)

    for e in range(max(local - 2, 0), local):
        hidden_relay(e)

    @pl.loop(0, local)
    def _(e):
        for dx in range(n_tp):
            for dc in range(1, n_dp):
                hidden_arrived(e, lax.rem(x + dx, n_tp) * n_dp + lax.rem(c + dc, n_dp))

        def body(m):
            span = pl.ds(pl.multiple_of(m * mt, mt), mt)
            slot = pl.ds(pl.multiple_of(m * ms, ms), ms)
            spread = jnp.dot(
                places(e, span), packed[e, slot, :], preferred_element_type=jnp.float32
            )
            hid[e, span, :] = spread.astype(jnp.bfloat16)

        each_m(body)

    for j in range(tiles):
        down_in(j).wait()

        def body(m):
            span = pl.ds(pl.multiple_of(m * mt, mt), mt)

            def add(e, total):
                return total + jnp.dot(
                    hid[e, span, :], dbuf[j, e], preferred_element_type=jnp.float32
                )

            total = lax.fori_loop(0, local, add, jnp.zeros((mt, tile), jnp.float32))
            pbuf[j, pl.ds(m * mb, mb)] = total.reshape(mb, rows, tile).astype(jnp.bfloat16)

        each_m(body)
        pltpu.make_async_copy(pbuf.at[j, me], back.at[j, z, q], pr_sem.at[j]).start()

        def give(a, b, d):
            pltpu.make_async_remote_copy(
                src_ref=pbuf.at[j, a * nq + b * n_dp + d],
                dst_ref=back.at[j, z, q],
                send_sem=ps_sem.at[j],
                recv_sem=pr_sem.at[j],
                device_id={"ep": a, "tp": b, "dp": d},
                device_id_type=MESH,
            ).start()

        others(give)

    for j in range(tiles):
        pltpu.make_async_copy(back.at[j], back.at[j], pr_sem.at[j]).wait()
        for qs in range(nq):
            total = back[j, 0, qs].astype(jnp.float32)
            for a in range(1, n_ep):
                total = total + back[j, a, qs].astype(jnp.float32)
            at = (qs * tiles + j) * tile
            out[:, at : at + tile] = total.astype(jnp.bfloat16)

    for k in range(chunks):
        sent = xr.at[k, pl.ds(0, nb - 1)]
        pltpu.make_async_copy(sent, sent, xs_sem.at[k]).wait()
    for e in range(local):
        sent = packed.at[e, :, pl.ds(0, (nq - 1) * ff)]
        pltpu.make_async_copy(sent, sent, hs_sem.at[e]).wait()
    for j in range(tiles):
        sent = pbuf.at[j, pl.ds(0, nb - 1)]
        pltpu.make_async_copy(sent, sent, ps_sem.at[j]).wait()


def per_device(tokens, route_weights, expert_ids, gate_weight, up_weight, down_weight):
    n_ep, n_tp, n_dp = (lax.axis_size(name) for name in ("ep", "tp", "dp"))
    nq = n_tp * n_dp
    nb = n_ep * nq
    rows, width = tokens.shape
    local, _, ff = gate_weight.shape
    _, full, part = down_weight.shape
    experts = local * n_ep
    ext = -(-3 * experts // LANES) * LANES
    chunks = CHUNKS if width % (CHUNKS * LANES) == 0 else 1
    depth = width // chunks
    slots = min(SLOTS, chunks * local)
    tile = 2 * LANES if part % (2 * LANES) == 0 else LANES
    tiles = part // tile
    count = nb * rows
    in_vmem = pl.BlockSpec(memory_space=pltpu.VMEM)
    any_space = pl.BlockSpec(memory_space=pl.ANY)
    dma = pltpu.SemaphoreType.DMA
    bf16 = jnp.bfloat16
    return pl.pallas_call(
        functools.partial(kernel, (n_ep, n_tp, n_dp, experts)),
        out_shape=jax.ShapeDtypeStruct((rows, width), bf16),
        in_specs=[in_vmem] * 3 + [any_space] * 3,
        out_specs=in_vmem,
        scratch_shapes=[
            pltpu.VMEM((chunks, rows, depth + ext), bf16),
            pltpu.VMEM((chunks, nb, rows, depth + ext), bf16),
            pltpu.VMEM((chunks, count, depth), bf16),
            pltpu.VMEM((slots, depth, ff), bf16),
            pltpu.VMEM((slots, depth, ff), bf16),
            pltpu.VMEM((tiles, local, full, tile), bf16),
            pltpu.VMEM((local, count, 2 * ff), jnp.float32),
            pltpu.VMEM((local, nb * CAP, full), bf16),
            pltpu.VMEM((local, count, full), bf16),
            pltpu.VMEM((count, ext), jnp.float32),
            pltpu.VMEM((tiles, nb, rows, tile), bf16),
            pltpu.VMEM((tiles, n_ep, nq, rows, tile), bf16),
            dma((slots,)),
            dma((slots,)),
            dma((tiles,)),
            dma,
            dma((chunks,)),
            dma((chunks, nb)),
            dma((local,)),
            dma((local, nq)),
            dma((tiles,)),
            dma((tiles,)),
        ],
        compiler_params=pltpu.CompilerParams(
            collective_id=0, has_side_effects=True, vmem_limit_bytes=67043328
        ),
        name="experts",
    )(tokens, route_weights, expert_ids, gate_weight, up_weight, down_weight)


def solution(mesh):
    rows = P(("groups", "ep", "tp", "dp"), None)
    weights = P("ep", None, ("tp", "dp"))
    return jax.shard_map(
        per_device,
        mesh=mesh,
        in_specs=(rows, rows, rows, weights, weights, weights),
        out_specs=rows,
        check_vma=False,
    )
```

```python
import functools

import jax
import jax.numpy as jnp
from jax import lax
from jax.experimental import pallas as pl
from jax.experimental.pallas import tpu as pltpu
from jax.sharding import PartitionSpec as P

MESH = pl.DeviceIdType.MESH
LANES = 128
CHUNKS = 1
SLOTS = 6
CAP = 4


def rows_and_routes(tokens, route_weights, expert_ids, xin, experts):
    chunks, rows, wide = xin.shape
    depth = tokens.shape[1] // chunks
    weight, ids = route_weights[...], expert_ids[...]
    lane = lax.broadcasted_iota(jnp.int32, (rows, wide - depth), 1)
    side = jnp.zeros((rows, wide - depth), jnp.float32)
    for term in range(3):
        held = weight.astype(jnp.bfloat16).astype(jnp.float32)
        weight = weight - held
        for k in range(ids.shape[1]):
            hit = lane == ids[:, k : k + 1] + term * experts
            side = side + jnp.where(hit, held[:, k : k + 1], 0.0)
    for k in range(chunks):
        xin[k, :, :depth] = tokens[:, k * depth : (k + 1) * depth]
        xin[k, :, depth:] = side.astype(jnp.bfloat16)


def kernel(
    dims,
    tokens,
    route_weights,
    expert_ids,
    gate_hbm,
    up_hbm,
    down_hbm,
    out,
    xin,
    xr,
    x2,
    gbuf,
    ubuf,
    dbuf,
    acc,
    packed,
    hid,
    ranks,
    offsets,
    pbuf,
    back,
    g_sem,
    u_sem,
    d_sem,
    own_sem,
    xs_sem,
    xr_sem,
    hs_sem,
    hr_sem,
    ps_sem,
    pr_sem,
):
    n_ep, n_tp, n_dp, experts = dims
    nq = n_tp * n_dp
    nb = n_ep * nq
    chunks, _, rows, _ = xr.shape
    _, count, depth = x2.shape
    slots = gbuf.shape[0]
    local = acc.shape[0]
    ff = gbuf.shape[2]
    tiles, _, full, tile = dbuf.shape
    units = chunks * local
    groups = 2 if local % 4 == 0 else 1
    ge = local // groups
    packed_rows = packed.shape[1]
    mt = min(count, 128)
    mb = mt // rows
    msteps = count // mt
    ms = packed_rows // msteps

    z, x, c = lax.axis_index("ep"), lax.axis_index("tp"), lax.axis_index("dp")
    q = x * n_dp + c
    me = z * nq + q

    def weights_in(u):
        k, e = u % (chunks * ge) // ge, u // (chunks * ge) * ge + u % ge
        s = u % slots
        span = pl.ds(pl.multiple_of(k * depth, depth), depth)
        return (
            pltpu.make_async_copy(gate_hbm.at[e, span, :], gbuf.at[s], g_sem.at[s]),
            pltpu.make_async_copy(up_hbm.at[e, span, :], ubuf.at[s], u_sem.at[s]),
        )

    def down_in(j):
        return pltpu.make_async_copy(
            down_hbm.at[:, :, j * tile : (j + 1) * tile], dbuf.at[j], d_sem.at[j]
        )

    for u in range(min(slots, units)):
        for copy in weights_in(u):
            copy.start()
    if units <= slots:
        for j in range(tiles):
            down_in(j).start()
    rows_and_routes(tokens, route_weights, expert_ids, xin, experts)
    own = pltpu.make_async_copy(xin, xr.at[:, me], own_sem)
    own.start()

    barrier = pltpu.get_barrier_semaphore()

    def others(act):
        for dz in range(n_ep):
            for dx in range(n_tp):
                for dc in range(n_dp):
                    if dz or dx or dc:
                        act(lax.rem(z + dz, n_ep), lax.rem(x + dx, n_tp), lax.rem(c + dc, n_dp))

    others(
        lambda a, b, d: pl.semaphore_signal(
            barrier, inc=1, device_id={"ep": a, "tp": b, "dp": d}, device_id_type=MESH
        )
    )
    pl.semaphore_wait(barrier, nb - 1)

    def pass_block(k, block, src, a, b, d):
        pltpu.make_async_remote_copy(
            src_ref=src,
            dst_ref=xr.at[k, block],
            send_sem=xs_sem.at[k],
            recv_sem=xr_sem.at[k, block],
            device_id={"ep": a, "tp": b, "dp": d},
            device_id_type=MESH,
        ).start()

    def arrived(k, block):
        pltpu.make_async_copy(xr.at[k, block], xr.at[k, block], xr_sem.at[k, block]).wait()

    order = []
    for s in range(1, n_ep // 2 + 1):
        order.append(s)
        if n_ep - s != s:
            order.append(n_ep - s)

    def to_tp(k, block, src):
        for dx in range(1, n_tp):
            pass_block(k, block, src, z, lax.rem(x + dx, n_tp), c)

    def to_dp(k, block, src):
        for dc in range(1, n_dp):
            pass_block(k, block, src, z, x, lax.rem(c + dc, n_dp))

    for k in range(chunks):
        for s in order:
            pass_block(k, me, xin.at[k], lax.rem(z + s, n_ep), x, c)
        to_tp(k, me, xin.at[k])
        to_dp(k, me, xin.at[k])

    def ep_steps(k):
        for s in order:
            block = lax.rem(z + n_ep - s, n_ep) * nq + q
            arrived(k, block)
            to_tp(k, block, xr.at[k, block])
            to_dp(k, block, xr.at[k, block])

    def tp_steps(k):
        for s in [0] + order:
            for dx in range(1, n_tp):
                block = lax.rem(z + n_ep - s, n_ep) * nq + lax.rem(x + dx, n_tp) * n_dp + c
                arrived(k, block)
                to_dp(k, block, xr.at[k, block])

    def dp_steps(k):
        for s in [0] + order:
            for dx in range(n_tp):
                for dc in range(1, n_dp):
                    block = (
                        lax.rem(z + n_ep - s, n_ep) * nq
                        + lax.rem(x + dx, n_tp) * n_dp
                        + lax.rem(c + dc, n_dp)
                    )
                    arrived(k, block)

    def each_m(body):
        if msteps == 1:
            body(0)
        else:

            @pl.loop(0, msteps)
            def _(m):
                body(m)

    def repack(k):
        def body(m):
            part = xr[k, pl.ds(m * mb, mb), :, :depth].astype(jnp.float32)
            x2[k, pl.ds(pl.multiple_of(m * mt, mt), mt), :] = part.reshape(mt, depth).astype(
                jnp.bfloat16
            )

        each_m(body)

    def routes(k, m):
        side = xr[k, pl.ds(m * mb, mb), :, depth:].astype(jnp.float32)
        return side.reshape(mt, side.shape[2])

    def rank_rows(k):
        row = lax.broadcasted_iota(jnp.int32, (mt, ms), 0)
        slot = lax.broadcasted_iota(jnp.int32, (mt, ms), 1)
        offset = slot - lax.div(row, rows) * CAP
        offsets[...] = offset.astype(jnp.float32)

        def body(m):
            named = (routes(k, m) > 0.0).astype(jnp.float32)
            row = lax.broadcasted_iota(jnp.int32, (mt, mt), 0)
            col = lax.broadcasted_iota(jnp.int32, (mt, mt), 1)
            before = (col < row) & (col >= row - lax.rem(row, rows))
            count_before = jnp.dot(
                before.astype(jnp.float32).astype(jnp.bfloat16),
                named.astype(jnp.bfloat16),
                preferred_element_type=jnp.float32,
            )
            ranks[pl.ds(pl.multiple_of(m * mt, mt), mt), :] = jnp.where(
                named > 0.0, count_before, -float(packed_rows)
            )

        each_m(body)

    def places(e, span):
        table = ranks[span, :]
        lane = lax.broadcasted_iota(jnp.int32, table.shape, 1)
        rank = jnp.sum(jnp.where(lane == z * local + e, table, 0.0), axis=1, keepdims=True)
        return jnp.where(offsets[...] == rank, 1.0, 0.0).astype(jnp.bfloat16)

    def hidden_to(e, qs, b, d):
        cols = pl.ds(pl.multiple_of(qs * ff, ff), ff)
        pltpu.make_async_remote_copy(
            src_ref=packed.at[e, :, cols],
            dst_ref=packed.at[e, :, cols],
            send_sem=hs_sem.at[e],
            recv_sem=hr_sem.at[e, qs],
            device_id={"ep": z, "tp": b, "dp": d},
            device_id_type=MESH,
        ).start()

    def hidden_arrived(e, qs):
        cols = pl.ds(pl.multiple_of(qs * ff, ff), ff)
        pltpu.make_async_copy(packed.at[e, :, cols], packed.at[e, :, cols], hr_sem.at[e, qs]).wait()

    def hidden_relay(e):
        for dx in range(1, n_tp):
            qs = lax.rem(x + dx, n_tp) * n_dp + c
            hidden_arrived(e, qs)
            for dc in range(1, n_dp):
                hidden_to(e, qs, x, lax.rem(c + dc, n_dp))

    def unit(k, e):
        u = e // ge * (chunks * ge) + k * ge + e % ge
        s = lax.rem(u, slots)
        for copy in weights_in(u):
            copy.wait()

        def body(m):
            span = pl.ds(pl.multiple_of(m * mt, mt), mt)
            gate = jnp.dot(x2[k, span, :], gbuf[s], preferred_element_type=jnp.float32)
            up = jnp.dot(x2[k, span, :], ubuf[s], preferred_element_type=jnp.float32)
            if k > 0:
                gate = gate + acc[e, span, :ff]
                up = up + acc[e, span, ff:]
            if k < chunks - 1:
                acc[e, span, :ff] = gate
                acc[e, span, ff:] = up
            else:
                side = routes(k, m)
                named = z * local + e
                lane = lax.broadcasted_iota(jnp.int32, side.shape, 1)
                mine = (lane == named) | (lane == named + experts) | (lane == named + 2 * experts)
                weight = jnp.sum(jnp.where(mine, side, 0.0), axis=1, keepdims=True)
                hidden = gate / (1.0 + jnp.exp(-gate)) * up * weight
                kept = lax.dot_general(
                    places(e, span),
                    hidden.astype(jnp.bfloat16),
                    (((0,), (0,)), ((), ())),
                    preferred_element_type=jnp.float32,
                )
                cols = pl.ds(pl.multiple_of(q * ff, ff), ff)
                slot = pl.ds(pl.multiple_of(m * ms, ms), ms)
                packed[e, slot, cols] = kept.astype(jnp.bfloat16)

        each_m(body)
        if units > slots:

            @pl.when(u + slots < units)
            def _():
                for copy in weights_in(u + slots):
                    copy.start()

            @pl.when(u == units - slots - 1)
            def _():
                for j in range(tiles):
                    down_in(j).start()

        if k == chunks - 1:
            for dx in range(1, n_tp):
                hidden_to(e, q, lax.rem(x + dx, n_tp), c)
            for dc in range(1, n_dp):
                hidden_to(e, q, x, lax.rem(c + dc, n_dp))

    ep_steps(0)
    tp_steps(0)
    own.wait()
    dp_steps(0)
    repack(0)
    rank_rows(0)
    for g in range(groups):
        for k in range(chunks):
            last = k == chunks - 1
            ahead = g == 0 and not last

            @pl.loop(0, ge)
            def _(i):
                unit(k, g * ge + i)
                if ahead and ge >= 4:
                    pl.when(i == 0)(lambda: ep_steps(k + 1))
                    pl.when(i == 2)(lambda: tp_steps(k + 1))
                if g > 0 and k == 0:
                    pl.when(i < 2)(lambda: hidden_relay(g * ge - 2 + i))
                if last and ge >= 2:
                    pl.when(i >= 2)(lambda: hidden_relay(g * ge + i - 2))

            if ahead:
                if ge < 4:
                    ep_steps(k + 1)
                    tp_steps(k + 1)
                dp_steps(k + 1)
                repack(k + 1)

    for e in range(max(local - 2, 0), local):
        hidden_relay(e)

    @pl.loop(0, local)
    def _(e):
        for dx in range(n_tp):
            for dc in range(1, n_dp):
                hidden_arrived(e, lax.rem(x + dx, n_tp) * n_dp + lax.rem(c + dc, n_dp))

        def body(m):
            span = pl.ds(pl.multiple_of(m * mt, mt), mt)
            slot = pl.ds(pl.multiple_of(m * ms, ms), ms)
            spread = jnp.dot(
                places(e, span), packed[e, slot, :], preferred_element_type=jnp.float32
            )
            hid[e, span, :] = spread.astype(jnp.bfloat16)

        each_m(body)

    for j in range(tiles):
        down_in(j).wait()

        def body(m):
            span = pl.ds(pl.multiple_of(m * mt, mt), mt)

            def add(e, total):
                return total + jnp.dot(
                    hid[e, span, :], dbuf[j, e], preferred_element_type=jnp.float32
                )

            total = lax.fori_loop(0, local, add, jnp.zeros((mt, tile), jnp.float32), unroll=True)
            pbuf[j, pl.ds(m * mb, mb)] = total.reshape(mb, rows, tile).astype(jnp.bfloat16)

        each_m(body)
        pltpu.make_async_copy(pbuf.at[j, me], back.at[j, z, q], pr_sem.at[j]).start()

        def give(a, b, d):
            pltpu.make_async_remote_copy(
                src_ref=pbuf.at[j, a * nq + b * n_dp + d],
                dst_ref=back.at[j, z, q],
                send_sem=ps_sem.at[j],
                recv_sem=pr_sem.at[j],
                device_id={"ep": a, "tp": b, "dp": d},
                device_id_type=MESH,
            ).start()

        others(give)

    for j in range(tiles):
        pltpu.make_async_copy(back.at[j], back.at[j], pr_sem.at[j]).wait()
        for qs in range(nq):
            total = back[j, 0, qs].astype(jnp.float32)
            for a in range(1, n_ep):
                total = total + back[j, a, qs].astype(jnp.float32)
            at = (qs * tiles + j) * tile
            out[:, at : at + tile] = total.astype(jnp.bfloat16)

    for k in range(chunks):
        sent = xr.at[k, pl.ds(0, nb - 1)]
        pltpu.make_async_copy(sent, sent, xs_sem.at[k]).wait()
    for e in range(local):
        sent = packed.at[e, :, pl.ds(0, (nq - 1) * ff)]
        pltpu.make_async_copy(sent, sent, hs_sem.at[e]).wait()
    for j in range(tiles):
        sent = pbuf.at[j, pl.ds(0, nb - 1)]
        pltpu.make_async_copy(sent, sent, ps_sem.at[j]).wait()


def per_device(tokens, route_weights, expert_ids, gate_weight, up_weight, down_weight):
    n_ep, n_tp, n_dp = (lax.axis_size(name) for name in ("ep", "tp", "dp"))
    nq = n_tp * n_dp
    nb = n_ep * nq
    rows, width = tokens.shape
    local, _, ff = gate_weight.shape
    _, full, part = down_weight.shape
    experts = local * n_ep
    ext = -(-3 * experts // LANES) * LANES
    chunks = CHUNKS if width % (CHUNKS * LANES) == 0 else 1
    depth = width // chunks
    slots = min(SLOTS, chunks * local)
    tile = 2 * LANES if part % (2 * LANES) == 0 else LANES
    tiles = part // tile
    count = nb * rows
    in_vmem = pl.BlockSpec(memory_space=pltpu.VMEM)
    any_space = pl.BlockSpec(memory_space=pl.ANY)
    dma = pltpu.SemaphoreType.DMA
    bf16 = jnp.bfloat16
    return pl.pallas_call(
        functools.partial(kernel, (n_ep, n_tp, n_dp, experts)),
        out_shape=jax.ShapeDtypeStruct((rows, width), bf16),
        in_specs=[in_vmem] * 3 + [any_space] * 3,
        out_specs=in_vmem,
        scratch_shapes=[
            pltpu.VMEM((chunks, rows, depth + ext), bf16),
            pltpu.VMEM((chunks, nb, rows, depth + ext), bf16),
            pltpu.VMEM((chunks, count, depth), bf16),
            pltpu.VMEM((slots, depth, ff), bf16),
            pltpu.VMEM((slots, depth, ff), bf16),
            pltpu.VMEM((tiles, local, full, tile), bf16),
            pltpu.VMEM((local, count, 2 * ff), jnp.float32),
            pltpu.VMEM((local, nb * CAP, full), bf16),
            pltpu.VMEM((local, count, full), bf16),
            pltpu.VMEM((count, ext), jnp.float32),
            pltpu.VMEM((min(count, 128), min(count, 128) // rows * CAP), jnp.float32),
            pltpu.VMEM((tiles, nb, rows, tile), bf16),
            pltpu.VMEM((tiles, n_ep, nq, rows, tile), bf16),
            dma((slots,)),
            dma((slots,)),
            dma((tiles,)),
            dma,
            dma((chunks,)),
            dma((chunks, nb)),
            dma((local,)),
            dma((local, nq)),
            dma((tiles,)),
            dma((tiles,)),
        ],
        compiler_params=pltpu.CompilerParams(
            collective_id=0, has_side_effects=True, vmem_limit_bytes=67043328
        ),
        name="experts",
    )(tokens, route_weights, expert_ids, gate_weight, up_weight, down_weight)


def solution(mesh):
    rows = P(("groups", "ep", "tp", "dp"), None)
    weights = P("ep", None, ("tp", "dp"))
    return jax.shard_map(
        per_device,
        mesh=mesh,
        in_specs=(rows, rows, rows, weights, weights, weights),
        out_specs=rows,
        check_vma=False,
    )
```
